16 devices in a mesh: dp: 2 (over y, z), tp: 8 (over x, core).
Axes of the slice: x: 4, y: 2, z: 1, core: 2. Of those that a mesh axis runs over, the one named last changes fastest.
The devices are a block of a 4x4x8 slice.
Arguments:
- x: bfloat16 [4096, 4096], P(('dp', 'tp')), parts along dimension 0
- w_gate: bfloat16 [4096, 12288], P(None, 'tp')
- w_up: bfloat16 [4096, 12288], P(None, 'tp')
- w_down: bfloat16 [12288, 4096], P('tp')
Outputs:
- output: bfloat16 [4096, 4096], P(('dp', 'tp')), parts along dimension 0
There are 2 independent parts. The reference program is written for one: setup_inputs(seed, part) draws one part's arguments, and reference() takes and returns one part's arrays. A program takes and returns all parts, laid end to end along the dimension named above; an argument that names none is the same for every part.
All inputs are finite; a program needn't handle non-finite values.
Results may differ from the reference program's by a relative error of at most 0.016.
Values are sent between devices in bfloat16 or wider.
A program may use at most 768 MiB of HBM per device.

```python
import jax
import jax.numpy as jnp

ROWS = 2048
D = 4096
FF = 12288


def setup_inputs(seed: int = 0, part: int = 0) -> dict:
    kx, kg, ku, kd = jax.random.split(jax.random.key(seed), 4)
    drawn = {
        "x": jax.random.normal(jax.random.fold_in(kx, part), (ROWS, D), jnp.float32),
        "w_gate": jax.random.normal(kg, (D, FF), jnp.float32) * D**-0.5,
        "w_up": jax.random.normal(ku, (D, FF), jnp.float32) * D**-0.5,
        "w_down": jax.random.normal(kd, (FF, D), jnp.float32) * FF**-0.5,
    }
    return {k: v.astype(jnp.bfloat16) for k, v in drawn.items()}


def reference(x, w_gate, w_up, w_down):
    gate = jnp.dot(x, w_gate, preferred_element_type=jnp.float32)
    up = jnp.dot(x, w_up, preferred_element_type=jnp.float32)
    hidden = (jax.nn.silu(gate) * up).astype(jnp.bfloat16)
    return jnp.dot(hidden, w_down, preferred_element_type=jnp.float32).astype(jnp.bfloat16)
```

```python
import functools

import jax
import jax.numpy as jnp
from jax import lax
from jax.experimental import pallas as pl
from jax.experimental.pallas import tpu as pltpu
from jax.sharding import PartitionSpec as P

MESH = pl.DeviceIdType.MESH
AXIS = "tp"
F32 = jnp.float32
BF16 = jnp.bfloat16
VMEM_BYTES = 67043328


def split(total, most):
    return max(t for t in range(256, min(total, most) + 1, 256) if total % t == 0)


def kernel(
    n,
    x, wg, wu, wd,
    y, xg, tp,
    wgv, wuv, wdv, xv, hv, ov, tv, sv, fv, own,
    w_sem, wd_sem, x_sem, t_sem, y_sem,
    ag_send, ag_recv, xd_send, xd_recv, td_send, td_recv,
    dir_send, dir_recv, far_send, far_recv, sum_send, sum_recv,
):
    rows, depth = x.shape
    ff = wg.shape[1]
    h, q = rows // 2, rows // 4
    me = lax.axis_index(AXIS)
    chips = n // 2
    c, k = lax.div(me, 2), lax.rem(me, 2)

    def device(step, core):
        return lax.rem(c + step + chips, chips) * 2 + core

    other = 1 - k
    partner = device(0, other)
    right, left = device(1, k), device(-1, k)
    to = (right, left)
    came = (left, right)

    def at(ref, block, start, size):
        return ref.at[block, pl.ds(start, size), :]

    def remote(src, dst, ssem, rsem, device_id):
        return pltpu.make_async_remote_copy(
            src_ref=src, dst_ref=dst, send_sem=ssem, recv_sem=rsem,
            device_id={AXIS: device_id}, device_id_type=MESH,
        )

    def first(d, j):
        return (0 if d == 0 else h) + j * q

    def second(d, j):
        return (h if d == 0 else 0) + j * q

    def ag(d, t):
        if t in (2, 3):
            r = pl.ds(first(d, t - 2), q)
            src = xg.at[came[d], r, :]
            dst = src
        else:
            r = pl.ds(first(d, t) if t < 2 else second(d, t - 4), q)
            src = x.at[r, :]
            dst = xg.at[me, r, :]
        return remote(src, dst, ag_send.at[d, t], ag_recv.at[d, t], to[d])

    def ag_wait(*ts):
        for t in ts:
            for d in (0, 1):
                ag(d, t).wait_recv()

    def ag_start(*ts):
        for t in ts:
            for d in (0, 1):
                ag(d, t).start()

    far = device(2, k)
    pieces = ((left, 0), (right, h), (far, 0), (far, h), (left, h), (right, 0))

    def xd(i):
        if i == 0:
            src, dst = x, xg.at[me]
        else:
            block, start = pieces[i - 1]
            src = at(xg, block, start, h)
            dst = src
        return remote(src, dst, xd_send.at[i], xd_recv.at[i], partner)

    def td(j, slot):
        return remote(ov.at[slot], tp.at[j], td_send.at[j], td_recv.at[j], partner)

    def direct(d):
        r = pl.ds(h, h) if d == 0 else pl.ds(0, h)
        return remote(ov.at[2, r, :], fv.at[d, r, :], dir_send.at[d], dir_recv.at[d], to[d])

    def distant(d, j):
        return remote(
            at(ov, 1, first(d, j), q), at(sv, d, j * q, q), far_send.at[d, j], far_recv.at[d, j], to[d]
        )

    def summed(d, j):
        return remote(
            at(ov, 2, (2 * j + d) * q, q), at(fv, d, first(d, j), q), sum_send.at[d, j], sum_recv.at[d, j], to[d]
        )

    def load(slot, parts):
        out, place = [], 0
        for i, (src, size) in enumerate(parts):
            out.append(pltpu.make_async_copy(src, xv.at[slot, pl.ds(place, size), :], x_sem.at[slot, i]))
            place += size
        return out

    def near(core):
        return [(at(xg, device(-1, core), 0, h), h), (at(xg, device(1, core), h, h), h)]

    def opposite(core):
        return [(xg.at[device(2, core)], rows)]

    def late(core):
        a, b = device(1, core), device(-1, core)
        return [(at(xg, a, 0, q), q), (at(xg, b, h, q), q), (at(xg, a, q, q), q), (at(xg, b, h + q, q), q)]

    def start(copies):
        for copy in copies:
            copy.start()

    def wait(copies):
        for copy in copies:
            copy.wait()

    def term(j):
        return pltpu.make_async_copy(tp.at[j], tv, t_sem)

    nt = split(ff, 768)
    dt = split(depth, 2048)

    def weights(i):
        r = pl.ds(pl.multiple_of(i * nt, nt), nt)
        return [
            pltpu.make_async_copy(wg.at[:, r], wgv.at[:, r], w_sem.at[0, i]),
            pltpu.make_async_copy(wu.at[:, r], wuv.at[:, r], w_sem.at[1, i]),
        ]

    down = pltpu.make_async_copy(wd, wdv, wd_sem)

    def up(slot, hslot, hook=None, arriving=False):
        def body(i, carry):
            if arriving:
                wait(weights(i))
            if hook is not None:
                pl.when(i == ff // nt - 1)(hook)
            for s in range(0, nt, 256):
                r = pl.ds(pl.multiple_of(i * nt + s, 256), 256)
                a = xv[slot]
                g = jnp.dot(a, wgv[:, r], preferred_element_type=F32)
                u = jnp.dot(a, wuv[:, r], preferred_element_type=F32)
                hv[hslot, :, r] = (g * jax.nn.sigmoid(g) * u).astype(BF16)
            return carry

        lax.fori_loop(0, ff // nt, body, 0)

    def project(hslot, place, size, finish, hook=None):
        def body(i, carry):
            if hook is not None:
                pl.when(i == depth // dt - 1)(hook)
            for s in range(0, dt, 512):
                r = pl.ds(pl.multiple_of(i * dt + s, 512), 512)
                finish(r, jnp.dot(hv[hslot, pl.ds(place, size), :], wdv[:, r], preferred_element_type=F32))
            return carry

        lax.fori_loop(0, depth // dt, body, 0)

    def to_other(slot):
        def finish(r, acc):
            ov[slot, :, r] = acc.astype(BF16)
        return finish

    def to_own(r, acc):
        own[:, r] = acc + tv[:, r].astype(F32)

    def to_ring(slot):
        def finish(r, acc):
            ov[slot, :, r] = (acc + tv[:, r].astype(F32)).astype(BF16)
        return finish

    def to_last(j):
        def finish(r, acc):
            for d in (0, 1):
                place = pl.ds((2 * j + d) * q, q)
                total = acc[d * q:(d + 1) * q] + tv[place, r].astype(F32) + sv[d, pl.ds(j * q, q), r].astype(F32)
                ov[2, place, r] = total.astype(BF16)
        return finish

    load_own = load(0, [(x, rows)])
    start(load_own)
    for i in range(ff // nt):
        start(weights(i))
    down.start()

    barrier = pltpu.get_barrier_semaphore()
    for device_id in (right, left, partner):
        pl.semaphore_signal(barrier, inc=1, device_id={AXIS: device_id}, device_id_type=MESH)
    pl.semaphore_wait(barrier, 3)

    ag_start(0, 1)
    xd(0).start()

    xd(0).wait_recv()
    load_partner = load(1, [(xg.at[partner], rows)])
    start(load_partner)
    wait(load_own)
    up(0, 0, arriving=True)

    ag_wait(0)
    ag_start(2)
    wait(load_partner)
    up(1, 1)
    down.wait()
    project(1, 0, rows, to_other(0))
    td(0, 0).start()

    ag_wait(1)
    ag_start(3, 4, 5)
    xd(1).start()
    xd(2).start()
    tile = load(0, near(k))
    start(tile)
    tile_other = load(1, near(other))

    def hook_near():
        xd(1).wait_recv()
        xd(2).wait_recv()
        start(tile_other)

    wait(tile)
    up(0, 1, hook_near)
    td(0, 0).wait_recv()
    term(0).start()
    wait(tile_other)
    up(1, 2)
    project(2, 0, rows, to_other(1))
    td(1, 1).start()
    term(0).wait()
    project(0, 0, rows, to_own)

    ag_wait(2, 3)
    xd(3).start()
    xd(4).start()
    td(1, 1).wait_recv()
    term(1).start()
    term(1).wait()
    tile_other2 = load(0, opposite(other))

    def hook_far():
        xd(3).wait_recv()
        xd(4).wait_recv()
        start(tile_other2)

    project(1, 0, rows, to_ring(2), hook_far)
    direct(0).start()
    direct(1).start()

    tile2 = load(1, opposite(k))
    start(tile2)
    wait(tile_other2)
    up(0, 0)
    td(0, 0).wait_send()
    project(0, 0, rows, to_other(0))
    td(2, 0).start()
    wait(tile2)
    up(1, 1)

    ag_wait(4, 5)
    xd(5).start()
    xd(6).start()
    td(2, 0).wait_recv()
    term(2).start()
    td(1, 1).wait_send()
    term(2).wait()
    tile_other3 = load(0, late(other))

    def hook_late():
        xd(5).wait_recv()
        xd(6).wait_recv()
        start(tile_other3)

    project(1, 0, rows, to_ring(1), hook_late)
    for j in (0, 1):
        for d in (0, 1):
            distant(d, j).start()

    tile3 = load(1, late(k))
    start(tile3)
    wait(tile_other3)
    up(0, 0)
    td(2, 0).wait_send()
    project(0, 0, rows, to_other(0))
    td(3, 0).start()
    wait(tile3)
    up(1, 1)
    td(3, 0).wait_recv()
    term(3).start()
    direct(0).wait_send()
    direct(1).wait_send()
    term(3).wait()

    for j in (0, 1):
        for d in (0, 1):
            distant(d, j).wait_recv()
        project(1, 2 * j * q, 2 * q, to_last(j))
        for d in (0, 1):
            summed(d, j).start()

    td(3, 0).wait_send()
    direct(0).wait_recv()
    direct(1).wait_recv()
    results = []
    for j in (0, 1):
        for d in (0, 1):
            summed(d, j).wait_recv()
            r = pl.ds(first(d, j), q)
            ov[0, r, :] = (own[r, :] + fv[0, r, :].astype(F32) + fv[1, r, :].astype(F32)).astype(BF16)
            copy = pltpu.make_async_copy(ov.at[0, r, :], y.at[r, :], y_sem.at[d, j])
            copy.start()
            results.append(copy)

    for t in range(6):
        for d in (0, 1):
            ag(d, t).wait_send()
    for i in range(7):
        xd(i).wait_send()
    for j in (0, 1):
        for d in (0, 1):
            distant(d, j).wait_send()
            summed(d, j).wait_send()
    wait(results)


def solution(mesh):
    n = mesh.shape[AXIS]

    def step(x, w_gate, w_up, w_down):
        rows, depth = x.shape
        ff = w_gate.shape[1]
        any_space = pl.BlockSpec(memory_space=pl.ANY)
        dma = pltpu.SemaphoreType.DMA
        out = pl.pallas_call(
            functools.partial(kernel, n),
            out_shape=(
                jax.ShapeDtypeStruct((rows, depth), BF16),
                jax.ShapeDtypeStruct((n, rows, depth), BF16),
                jax.ShapeDtypeStruct((n // 2, rows, depth), BF16),
            ),
            in_specs=[any_space] * 4,
            out_specs=(any_space,) * 3,
            scratch_shapes=[
                pltpu.VMEM((depth, ff), BF16),
                pltpu.VMEM((depth, ff), BF16),
                pltpu.VMEM((ff, depth), BF16),
                pltpu.VMEM((2, rows, depth), BF16),
                pltpu.VMEM((3, rows, ff), BF16),
                pltpu.VMEM((3, rows, depth), BF16),
                pltpu.VMEM((rows, depth), BF16),
                pltpu.VMEM((2, rows // 2, depth), BF16),
                pltpu.VMEM((2, rows, depth), BF16),
                pltpu.VMEM((rows, depth), F32),
                dma((2, ff // split(ff, 768))),
                dma,
                dma((2, 4)),
                dma,
                dma((2, 2)),
                dma((2, 6)), dma((2, 6)),
                dma((7,)), dma((7,)),
                dma((4,)), dma((4,)),
                dma((2,)), dma((2,)),
                dma((2, 2)), dma((2, 2)),
                dma((2, 2)), dma((2, 2)),
            ],
            compiler_params=pltpu.CompilerParams(
                collective_id=0, has_side_effects=True, vmem_limit_bytes=VMEM_BYTES
            ),
            name="mlp_block",
        )(x, w_gate, w_up, w_down)
        return out[0]

    return jax.shard_map(
        step,
        mesh=mesh,
        in_specs=(P(("dp", "tp"), None), P(None, "tp"), P(None, "tp"), P("tp", None)),
        out_specs=P(("dp", "tp"), None),
        check_vma=False,
    )
```

```python
import functools

import jax
import jax.numpy as jnp
from jax import lax
from jax.experimental import pallas as pl
from jax.experimental.pallas import tpu as pltpu
from jax.sharding import PartitionSpec as P

MESH = pl.DeviceIdType.MESH
AXIS = "tp"
F32 = jnp.float32
BF16 = jnp.bfloat16
VMEM_BYTES = 67043328 - 2 * 1024 * 1024


def split(total, most):
    return max(t for t in range(256, min(total, most) + 1, 256) if total % t == 0)


def kernel(
    n,
    x, wg, wu, wd,
    y, xg, tp,
    wgv, wuv, wdv, xv, hv, ov, tv, sv, fv, own,
    w_sem, wd_sem, x_sem, t_sem,
    ag_send, ag_recv, xd_send, xd_recv, td_send, td_recv,
    dir_send, dir_recv, far_send, far_recv, sum_send, sum_recv,
):
    rows, depth = x.shape
    ff = wg.shape[1]
    h, q = rows // 2, rows // 4
    me = lax.axis_index(AXIS)
    chips = n // 2
    c, k = lax.div(me, 2), lax.rem(me, 2)

    def device(step, core):
        return lax.rem(c + step + chips, chips) * 2 + core

    other = 1 - k
    partner = device(0, other)
    right, left = device(1, k), device(-1, k)
    to = (right, left)
    came = (left, right)

    def at(ref, block, start, size):
        return ref.at[block, pl.ds(start, size), :]

    def remote(src, dst, ssem, rsem, device_id):
        return pltpu.make_async_remote_copy(
            src_ref=src, dst_ref=dst, send_sem=ssem, recv_sem=rsem,
            device_id={AXIS: device_id}, device_id_type=MESH,
        )

    def first(d, j):
        return (0 if d == 0 else h) + j * q

    def second(d, j):
        return (h if d == 0 else 0) + j * q

    def ag(d, t):
        if t in (2, 3):
            r = pl.ds(first(d, t - 2), q)
            src = xg.at[came[d], r, :]
            dst = src
        else:
            r = pl.ds(first(d, t) if t < 2 else second(d, t - 4), q)
            src = x.at[r, :]
            dst = xg.at[me, r, :]
        return remote(src, dst, ag_send.at[d, t], ag_recv.at[d, t], to[d])

    def ag_wait(*ts):
        for t in ts:
            for d in (0, 1):
                ag(d, t).wait_recv()

    def ag_start(*ts):
        for t in ts:
            for d in (0, 1):
                ag(d, t).start()

    far = device(2, k)
    pieces = ((left, 0), (right, h), (far, 0), (far, h), (left, h), (right, 0))

    def xd(i):
        if i == 0:
            src, dst = x, xg.at[me]
        else:
            block, start = pieces[i - 1]
            src = at(xg, block, start, h)
            dst = src
        return remote(src, dst, xd_send.at[i], xd_recv.at[i], partner)

    def td(j, slot):
        return remote(ov.at[slot], tp.at[j], td_send.at[j], td_recv.at[j], partner)

    def direct(d):
        r = pl.ds(h, h) if d == 0 else pl.ds(0, h)
        return remote(ov.at[2, r, :], fv.at[d, r, :], dir_send.at[d], dir_recv.at[d], to[d])

    def distant(d, j):
        return remote(
            at(ov, 1, first(d, j), q), at(sv, d, j * q, q), far_send.at[d, j], far_recv.at[d, j], to[d]
        )

    def summed(d, j):
        return remote(
            at(ov, 2, (2 * j + d) * q, q), at(fv, d, first(d, j), q), sum_send.at[d, j], sum_recv.at[d, j], to[d]
        )

    def load(slot, parts):
        out, place = [], 0
        for i, (src, size) in enumerate(parts):
            out.append(pltpu.make_async_copy(src, xv.at[slot, pl.ds(place, size), :], x_sem.at[slot, i]))
            place += size
        return out

    def near(core):
        return [(at(xg, device(-1, core), 0, h), h), (at(xg, device(1, core), h, h), h)]

    def opposite(core):
        return [(xg.at[device(2, core)], rows)]

    def late(core):
        a, b = device(1, core), device(-1, core)
        return [(at(xg, a, 0, q), q), (at(xg, b, h, q), q), (at(xg, a, q, q), q), (at(xg, b, h + q, q), q)]

    def start(copies):
        for copy in copies:
            copy.start()

    def wait(copies):
        for copy in copies:
            copy.wait()

    def term(j):
        return pltpu.make_async_copy(tp.at[j], tv, t_sem)

    nt = split(ff, 768)
    dt = split(depth, 2048)

    def weights(i):
        r = pl.ds(pl.multiple_of(i * nt, nt), nt)
        return [
            pltpu.make_async_copy(wg.at[:, r], wgv.at[:, r], w_sem.at[0, i]),
            pltpu.make_async_copy(wu.at[:, r], wuv.at[:, r], w_sem.at[1, i]),
        ]

    down = pltpu.make_async_copy(wd, wdv, wd_sem)

    def up(slot, hslot, hook=None, arriving=False):
        def body(i, carry):
            if arriving:
                wait(weights(i))
            if hook is not None:
                pl.when(i == ff // nt - 1)(hook)
            for s in range(0, nt, 256):
                r = pl.ds(pl.multiple_of(i * nt + s, 256), 256)
                a = xv[slot]
                g = jnp.dot(a, wgv[:, r], preferred_element_type=F32)
                u = jnp.dot(a, wuv[:, r], preferred_element_type=F32)
                hv[hslot, :, r] = (g * jax.nn.sigmoid(g) * u).astype(BF16)
            return carry

        lax.fori_loop(0, ff // nt, body, 0)

    def project(hslot, place, size, finish, hook=None):
        def body(i, carry):
            if hook is not None:
                pl.when(i == depth // dt - 1)(hook)
            for s in range(0, dt, 512):
                r = pl.ds(pl.multiple_of(i * dt + s, 512), 512)
                finish(r, jnp.dot(hv[hslot, pl.ds(place, size), :], wdv[:, r], preferred_element_type=F32))
            return carry

        lax.fori_loop(0, depth // dt, body, 0)

    def to_other(slot):
        def finish(r, acc):
            ov[slot, :, r] = acc.astype(BF16)
        return finish

    def to_own(r, acc):
        own[:, r] = acc + tv[:, r].astype(F32)

    def to_ring(slot):
        def finish(r, acc):
            ov[slot, :, r] = (acc + tv[:, r].astype(F32)).astype(BF16)
        return finish

    def to_last(j):
        def finish(r, acc):
            for d in (0, 1):
                place = pl.ds((2 * j + d) * q, q)
                total = acc[d * q:(d + 1) * q] + tv[place, r].astype(F32) + sv[d, pl.ds(j * q, q), r].astype(F32)
                ov[2, place, r] = total.astype(BF16)
        return finish

    barrier = pltpu.get_barrier_semaphore()
    for device_id in (right, left, partner):
        pl.semaphore_signal(barrier, inc=1, device_id={AXIS: device_id}, device_id_type=MESH)
    load_own = load(0, [(x, rows)])
    start(load_own)
    for i in range(ff // nt):
        start(weights(i))
    down.start()

    pl.semaphore_wait(barrier, 3)

    ag_start(0, 1)
    xd(0).start()

    xd(0).wait_recv()
    load_partner = load(1, [(xg.at[partner], rows)])
    start(load_partner)
    wait(load_own)
    up(0, 0, arriving=True)

    ag_wait(0)
    ag_start(2)
    wait(load_partner)
    up(1, 1)
    down.wait()
    project(1, 0, rows, to_other(0))
    td(0, 0).start()

    ag_wait(1)
    ag_start(3, 4, 5)
    xd(1).start()
    xd(2).start()
    tile = load(0, near(k))
    start(tile)
    tile_other = load(1, near(other))

    def hook_near():
        xd(1).wait_recv()
        xd(2).wait_recv()
        start(tile_other)

    wait(tile)
    up(0, 1, hook_near)
    td(0, 0).wait_recv()
    term(0).start()
    wait(tile_other)
    up(1, 2)
    project(2, 0, rows, to_other(1))
    td(1, 1).start()
    term(0).wait()
    project(0, 0, rows, to_own)

    ag_wait(2, 3)
    xd(3).start()
    xd(4).start()
    td(1, 1).wait_recv()
    term(1).start()
    term(1).wait()
    tile_other2 = load(0, opposite(other))

    def hook_far():
        xd(3).wait_recv()
        xd(4).wait_recv()
        start(tile_other2)

    project(1, 0, rows, to_ring(2), hook_far)
    direct(0).start()
    direct(1).start()

    tile2 = load(1, opposite(k))
    start(tile2)
    wait(tile_other2)
    up(0, 0)
    td(0, 0).wait_send()
    project(0, 0, rows, to_other(0))
    td(2, 0).start()
    wait(tile2)
    up(1, 1)

    ag_wait(4, 5)
    xd(5).start()
    xd(6).start()
    td(2, 0).wait_recv()
    term(2).start()
    td(1, 1).wait_send()
    term(2).wait()
    tile_other3 = load(0, late(other))

    def hook_late():
        xd(5).wait_recv()
        xd(6).wait_recv()
        start(tile_other3)

    project(1, 0, rows, to_ring(1), hook_late)
    for j in (0, 1):
        for d in (0, 1):
            distant(d, j).start()

    tile3 = load(1, late(k))
    start(tile3)
    wait(tile_other3)
    up(0, 0)
    td(2, 0).wait_send()
    project(0, 0, rows, to_other(0))
    td(3, 0).start()
    wait(tile3)
    up(1, 1)
    td(3, 0).wait_recv()
    term(3).start()
    direct(0).wait_send()
    direct(1).wait_send()
    term(3).wait()

    for j in (0, 1):
        for d in (0, 1):
            distant(d, j).wait_recv()
        project(1, 2 * j * q, 2 * q, to_last(j))
        for d in (0, 1):
            summed(d, j).start()

    td(3, 0).wait_send()
    for t in range(6):
        for d in (0, 1):
            ag(d, t).wait_send()
    for i in range(7):
        xd(i).wait_send()
    for j in (0, 1):
        for d in (0, 1):
            distant(d, j).wait_send()
    direct(0).wait_recv()
    direct(1).wait_recv()
    for j in (0, 1):
        for d in (0, 1):
            if j == 1:
                summed(d, 0).wait_send()
            summed(d, j).wait_recv()
            r = pl.ds(first(d, j), q)
            y[r, :] = (own[r, :] + fv[0, r, :].astype(F32) + fv[1, r, :].astype(F32)).astype(BF16)

    for d in (0, 1):
        summed(d, 1).wait_send()


def solution(mesh):
    n = mesh.shape[AXIS]

    def step(x, w_gate, w_up, w_down):
        rows, depth = x.shape
        ff = w_gate.shape[1]
        any_space = pl.BlockSpec(memory_space=pl.ANY)
        dma = pltpu.SemaphoreType.DMA
        out = pl.pallas_call(
            functools.partial(kernel, n),
            out_shape=(
                pltpu.VMEM((rows, depth), BF16),
                jax.ShapeDtypeStruct((n, rows, depth), BF16),
                jax.ShapeDtypeStruct((n // 2, rows, depth), BF16),
            ),
            in_specs=[any_space] * 4,
            out_specs=(pl.BlockSpec(memory_space=pltpu.VMEM), any_space, any_space),
            scratch_shapes=[
                pltpu.VMEM((depth, ff), BF16),
                pltpu.VMEM((depth, ff), BF16),
                pltpu.VMEM((ff, depth), BF16),
                pltpu.VMEM((2, rows, depth), BF16),
                pltpu.VMEM((3, rows, ff), BF16),
                pltpu.VMEM((3, rows, depth), BF16),
                pltpu.VMEM((rows, depth), BF16),
                pltpu.VMEM((2, rows // 2, depth), BF16),
                pltpu.VMEM((2, rows, depth), BF16),
                pltpu.VMEM((rows, depth), F32),
                dma((2, ff // split(ff, 768))),
                dma,
                dma((2, 4)),
                dma,
                dma((2, 6)), dma((2, 6)),
                dma((7,)), dma((7,)),
                dma((4,)), dma((4,)),
                dma((2,)), dma((2,)),
                dma((2, 2)), dma((2, 2)),
                dma((2, 2)), dma((2, 2)),
            ],
            compiler_params=pltpu.CompilerParams(
                collective_id=0, has_side_effects=True, vmem_limit_bytes=VMEM_BYTES
            ),
            name="mlp_block",
        )(x, w_gate, w_up, w_down)
        return out[0]

    return jax.shard_map(
        step,
        mesh=mesh,
        in_specs=(P(("dp", "tp"), None), P(None, "tp"), P(None, "tp"), P("tp", None)),
        out_specs=P(("dp", "tp"), None),
        check_vma=False,
    )
```

```python
import functools

import jax
import jax.numpy as jnp
from jax import lax
from jax.experimental import pallas as pl
from jax.experimental.pallas import tpu as pltpu
from jax.sharding import PartitionSpec as P

MESH = pl.DeviceIdType.MESH
AXIS = "tp"
F32 = jnp.float32
BF16 = jnp.bfloat16
VMEM_BYTES = 67043328 - 2 * 1024 * 1024


def split(total, most):
    return max(t for t in range(256, min(total, most) + 1, 256) if total % t == 0)


def kernel(
    n,
    x, wg, wu, wd,
    y, xg, tp,
    wgv, wuv, wdv, xv, hv, ov, tv, sv, fv, own,
    w_sem, wd_sem, x_sem, t_sem, rows_sent, sums_sent,
    ag_recv, xd_recv, td_send, td_recv, dir_send, dir_recv, far_recv, sum_recv,
):
    rows, depth = x.shape
    ff = wg.shape[1]
    h, q = rows // 2, rows // 4
    me = lax.axis_index(AXIS)
    chips = n // 2
    c, k = lax.div(me, 2), lax.rem(me, 2)

    def device(step, core):
        return lax.rem(c + step + chips, chips) * 2 + core

    other = 1 - k
    partner = device(0, other)
    right, left = device(1, k), device(-1, k)
    to = (right, left)
    came = (left, right)

    def at(ref, block, start, size):
        return ref.at[block, pl.ds(start, size), :]

    def remote(src, dst, ssem, rsem, device_id):
        return pltpu.make_async_remote_copy(
            src_ref=src, dst_ref=dst, send_sem=ssem, recv_sem=rsem,
            device_id={AXIS: device_id}, device_id_type=MESH,
        )

    def landed(sem, count):
        if count % rows == 0:
            ref = xg.at[pl.ds(0, count // rows)]
        else:
            ref = at(xg, 0, 0, count)
        pltpu.make_async_copy(ref, ref, sem).wait()

    def first(d, j):
        return (0 if d == 0 else h) + j * q

    def second(d, j):
        return (h if d == 0 else 0) + j * q

    def ag(d, t):
        if t in (2, 3):
            r = pl.ds(first(d, t - 2), q)
            src = xg.at[came[d], r, :]
            dst = src
        else:
            r = pl.ds(first(d, t), q) if t < 2 else pl.ds(second(d, 0), h)
            src = x.at[r, :]
            dst = xg.at[me, r, :]
        return remote(src, dst, rows_sent, ag_recv.at[(0, 1, 2, 2, 3)[t]], to[d])

    def ag_wait(i):
        landed(ag_recv.at[i], (2 * q, 2 * q, 4 * q, 2 * h)[i])

    def ag_start(*ts):
        for t in ts:
            for d in (0, 1):
                ag(d, t).start()

    far = device(2, k)
    pieces = ((left, 0), (right, h), (far, 0), (far, h), (left, h), (right, 0))

    def xd(i):
        if i == 0:
            src, dst = x, xg.at[me]
        else:
            block, start = pieces[i - 1]
            src = at(xg, block, start, h)
            dst = src
        return remote(src, dst, rows_sent, xd_recv.at[(i + 1) // 2], partner)

    def xd_wait(i):
        landed(xd_recv.at[i], rows)

    def td(j, slot):
        return remote(ov.at[slot], tp.at[j], td_send.at[slot], td_recv.at[j], partner)

    def direct(d):
        r = pl.ds(h, h) if d == 0 else pl.ds(0, h)
        return remote(ov.at[2, r, :], fv.at[d, r, :], dir_send, dir_recv, to[d])

    def distant(d, j):
        return remote(at(ov, 1, first(d, j), q), at(sv, d, j * q, q), sums_sent, far_recv.at[j], to[d])

    cuts = ((0, q), (q, q // 2), (q + q // 2, q // 2))

    def summed(d, i):
        place, size = cuts[i]
        src = at(ov, 2, (2 * (place // q) + d) * q + place % q, size)
        return remote(src, at(fv, d, first(d, 0) + place, size), sums_sent, sum_recv.at[i], to[d])

    def load(slot, parts):
        out, place = [], 0
        for src, size in parts:
            out.append(pltpu.make_async_copy(src, xv.at[slot, pl.ds(place, size), :], x_sem.at[slot]))
            place += size
        return out

    def near(core):
        return [(at(xg, device(-1, core), 0, h), h), (at(xg, device(1, core), h, h), h)]

    def opposite(core):
        return [(xg.at[device(2, core)], rows)]

    def late(core):
        a, b = device(1, core), device(-1, core)
        return [(at(xg, a, 0, q), q), (at(xg, b, h, q), q), (at(xg, a, q, q), q), (at(xg, b, h + q, q), q)]

    def start(copies):
        for copy in copies:
            copy.start()

    def wait(copies):
        for copy in copies:
            copy.wait()

    def loaded(slot):
        landed(x_sem.at[slot], rows)

    def term(j):
        return pltpu.make_async_copy(tp.at[j], tv, t_sem)

    nt = split(ff, 768)
    dt = split(depth, 2048)

    def weights(i):
        r = pl.ds(pl.multiple_of(i * nt, nt), nt)
        return [
            pltpu.make_async_copy(wg.at[:, r], wgv.at[:, r], w_sem.at[0, i]),
            pltpu.make_async_copy(wu.at[:, r], wuv.at[:, r], w_sem.at[1, i]),
        ]

    down = pltpu.make_async_copy(wd, wdv, wd_sem)

    def up(slot, hslot, hook=None, arriving=False):
        def body(i, carry):
            if arriving:
                wait(weights(i))
            if hook is not None:
                pl.when(i == ff // nt - 1)(hook)
            for s in range(0, nt, 256):
                r = pl.ds(pl.multiple_of(i * nt + s, 256), 256)
                a = xv[slot]
                g = jnp.dot(a, wgv[:, r], preferred_element_type=F32)
                u = jnp.dot(a, wuv[:, r], preferred_element_type=F32)
                hv[hslot, :, r] = (g * jax.nn.sigmoid(g) * u).astype(BF16)
            return carry

        lax.fori_loop(0, ff // nt, body, 0)

    def project(hslot, place, size, finish, hook=None):
        def body(i, carry):
            if hook is not None:
                pl.when(i == depth // dt - 1)(hook)
            for s in range(0, dt, 512):
                r = pl.ds(pl.multiple_of(i * dt + s, 512), 512)
                finish(r, jnp.dot(hv[hslot, pl.ds(place, size), :], wdv[:, r], preferred_element_type=F32))
            return carry

        lax.fori_loop(0, depth // dt, body, 0)

    def to_other(slot):
        def finish(r, acc):
            ov[slot, :, r] = acc.astype(BF16)
        return finish

    def to_own(r, acc):
        own[:, r] = acc + tv[:, r].astype(F32)

    def to_ring(slot):
        def finish(r, acc):
            ov[slot, :, r] = (acc + tv[:, r].astype(F32)).astype(BF16)
        return finish

    def to_last(j):
        def finish(r, acc):
            for d in (0, 1):
                place = pl.ds((2 * j + d) * q, q)
                total = acc[d * q:(d + 1) * q] + tv[place, r].astype(F32) + sv[d, pl.ds(j * q, q), r].astype(F32)
                ov[2, place, r] = total.astype(BF16)
        return finish

    barrier = pltpu.get_barrier_semaphore()
    for device_id in (right, left, partner):
        pl.semaphore_signal(barrier, inc=1, device_id={AXIS: device_id}, device_id_type=MESH)
    load_own = load(0, [(x, rows)])
    start(load_own)
    for i in range(ff // nt):
        start(weights(i))
    down.start()

    pl.semaphore_wait(barrier, 3)

    ag_start(0, 1)
    xd(0).start()

    xd_wait(0)
    load_partner = load(1, [(xg.at[partner], rows)])
    start(load_partner)
    loaded(0)
    up(0, 0, arriving=True)

    ag_wait(0)
    ag_start(2)
    loaded(1)
    up(1, 1)
    down.wait()
    project(1, 0, rows, to_other(0))
    td(0, 0).start()

    ag_wait(1)
    ag_start(3, 4)
    xd(1).start()
    xd(2).start()
    tile = load(0, near(k))
    start(tile)
    tile_other = load(1, near(other))

    def hook_near():
        xd_wait(1)
        start(tile_other)

    loaded(0)
    up(0, 1, hook_near)
    td(0, 0).wait_recv()
    term(0).start()
    loaded(1)
    up(1, 2)
    project(2, 0, rows, to_other(1))
    td(1, 1).start()
    term(0).wait()
    project(0, 0, rows, to_own)

    ag_wait(2)
    xd(3).start()
    xd(4).start()
    td(1, 1).wait_recv()
    term(1).start()
    term(1).wait()
    tile_other2 = load(0, opposite(other))

    def hook_far():
        xd_wait(2)
        start(tile_other2)

    project(1, 0, rows, to_ring(2), hook_far)
    direct(0).start()
    direct(1).start()

    tile2 = load(1, opposite(k))
    start(tile2)
    loaded(0)
    up(0, 0)
    td(0, 0).wait_send()
    project(0, 0, rows, to_other(0))
    td(2, 0).start()
    loaded(1)
    up(1, 1)

    ag_wait(3)
    xd(5).start()
    xd(6).start()
    td(2, 0).wait_recv()
    term(2).start()
    td(1, 1).wait_send()
    term(2).wait()
    tile_other3 = load(0, late(other))

    def hook_late():
        xd_wait(3)
        start(tile_other3)

    project(1, 0, rows, to_ring(1), hook_late)
    for j in (0, 1):
        for d in (0, 1):
            distant(d, j).start()

    tile3 = load(1, late(k))
    start(tile3)
    loaded(0)
    up(0, 0)
    td(2, 0).wait_send()
    project(0, 0, rows, to_other(0))
    td(3, 0).start()
    loaded(1)
    up(1, 1)
    td(3, 0).wait_recv()
    term(3).start()
    landed(dir_send, rows)
    term(3).wait()

    for j in (0, 1):
        landed(far_recv.at[j], 2 * q)
        project(1, 2 * j * q, 2 * q, to_last(j))
        for i in (0,) if j == 0 else (1, 2):
            for d in (0, 1):
                summed(d, i).start()

    td(3, 0).wait_send()
    landed(rows_sent, 3 * rows + 4 * rows)
    landed(dir_recv, rows)
    for i, (place, size) in enumerate(cuts):
        landed(sum_recv.at[i], 2 * size)
        for d in (0, 1):
            r = pl.ds(first(d, 0) + place, size)
            y[r, :] = (own[r, :] + fv[0, r, :].astype(F32) + fv[1, r, :].astype(F32)).astype(BF16)
    landed(sums_sent, 2 * rows)


def solution(mesh):
    n = mesh.shape[AXIS]

    def step(x, w_gate, w_up, w_down):
        rows, depth = x.shape
        ff = w_gate.shape[1]
        any_space = pl.BlockSpec(memory_space=pl.ANY)
        dma = pltpu.SemaphoreType.DMA
        out = pl.pallas_call(
            functools.partial(kernel, n),
            out_shape=(
                pltpu.VMEM((rows, depth), BF16),
                jax.ShapeDtypeStruct((n, rows, depth), BF16),
                jax.ShapeDtypeStruct((n // 2, rows, depth), BF16),
            ),
            in_specs=[any_space] * 4,
            out_specs=(pl.BlockSpec(memory_space=pltpu.VMEM), any_space, any_space),
            scratch_shapes=[
                pltpu.VMEM((depth, ff), BF16),
                pltpu.VMEM((depth, ff), BF16),
                pltpu.VMEM((ff, depth), BF16),
                pltpu.VMEM((2, rows, depth), BF16),
                pltpu.VMEM((3, rows, ff), BF16),
                pltpu.VMEM((3, rows, depth), BF16),
                pltpu.VMEM((rows, depth), BF16),
                pltpu.VMEM((2, rows // 2, depth), BF16),
                pltpu.VMEM((2, rows, depth), BF16),
                pltpu.VMEM((rows, depth), F32),
                dma((2, ff // split(ff, 768))), dma, dma((2,)), dma, dma, dma,
                dma((4,)), dma((4,)), dma((2,)), dma((4,)), dma, dma, dma((2,)), dma((3,)),
            ],
            compiler_params=pltpu.CompilerParams(
                collective_id=0, has_side_effects=True, vmem_limit_bytes=VMEM_BYTES
            ),
            name="mlp_block",
        )(x, w_gate, w_up, w_down)
        return out[0]

    return jax.shard_map(
        step,
        mesh=mesh,
        in_specs=(P(("dp", "tp"), None), P(None, "tp"), P(None, "tp"), P("tp", None)),
        out_specs=P(("dp", "tp"), None),
        check_vma=False,
    )
```

```python
import functools

import jax
import jax.numpy as jnp
from jax import lax
from jax.experimental import pallas as pl
from jax.experimental.pallas import tpu as pltpu
from jax.sharding import PartitionSpec as P

MESH = pl.DeviceIdType.MESH
AXIS = "tp"
F32 = jnp.float32
BF16 = jnp.bfloat16
VMEM_BYTES = 67043328 - 2 * 1024 * 1024


def split(total, most):
    return max(t for t in range(256, min(total, most) + 1, 256) if total % t == 0)


def kernel(
    n,
    x, wg, wu, wd,
    y, xg,
    wgv, wuv, wdv, xv, hv, ov, tv, sv, fv, own,
    w_sem, wd_sem, x_sem, rows_sent, sums_sent,
    ag_recv, xd_recv, td_send, td_recv, dir_send, dir_recv, far_recv, sum_recv,
):
    rows, depth = x.shape
    ff = wg.shape[1]
    h, q = rows // 2, rows // 4
    me = lax.axis_index(AXIS)
    chips = n // 2
    c, k = lax.div(me, 2), lax.rem(me, 2)

    def device(step, core):
        return lax.rem(c + step + chips, chips) * 2 + core

    other = 1 - k
    partner = device(0, other)
    right, left = device(1, k), device(-1, k)
    to = (right, left)
    came = (left, right)

    def at(ref, block, start, size):
        return ref.at[block, pl.ds(start, size), :]

    def remote(src, dst, ssem, rsem, device_id):
        return pltpu.make_async_remote_copy(
            src_ref=src, dst_ref=dst, send_sem=ssem, recv_sem=rsem,
            device_id={AXIS: device_id}, device_id_type=MESH,
        )

    def landed(sem, count):
        if count % rows == 0:
            ref = xg.at[pl.ds(0, count // rows)]
        else:
            ref = at(xg, 0, 0, count)
        pltpu.make_async_copy(ref, ref, sem).wait()

    def first(d, j):
        return (0 if d == 0 else h) + j * q

    def second(d, j):
        return (h if d == 0 else 0) + j * q

    def ag(d, t):
        if t in (2, 3):
            r = pl.ds(first(d, t - 2), q)
            src = xg.at[came[d], r, :]
            dst = src
        else:
            r = pl.ds(first(d, t), q) if t < 2 else pl.ds(second(d, 0), h)
            src = x.at[r, :]
            dst = xg.at[me, r, :]
        return remote(src, dst, rows_sent, ag_recv.at[(0, 1, 2, 2, 3)[t]], to[d])

    def ag_wait(i):
        landed(ag_recv.at[i], (2 * q, 2 * q, 4 * q, 2 * h)[i])

    def ag_start(*ts):
        for t in ts:
            for d in (0, 1):
                ag(d, t).start()

    far = device(2, k)
    pieces = ((left, 0), (right, h), (far, 0), (far, h), (left, h), (right, 0))

    def xd(i):
        if i == 0:
            src, dst = x, xg.at[me]
        else:
            block, start = pieces[i - 1]
            src = at(xg, block, start, h)
            dst = src
        return remote(src, dst, rows_sent, xd_recv.at[(i + 1) // 2], partner)

    def xd_wait(i):
        landed(xd_recv.at[i], rows)

    def td(j, slot):
        return remote(ov.at[slot], tv.at[j % 2], td_send.at[slot], td_recv.at[j], partner)

    def direct(d):
        r = pl.ds(h, h) if d == 0 else pl.ds(0, h)
        return remote(ov.at[2, r, :], fv.at[d, r, :], dir_send, dir_recv, to[d])

    def distant(d, j):
        return remote(at(ov, 1, first(d, j), q), at(sv, d, j * q, q), sums_sent, far_recv.at[j], to[d])

    cuts = ((0, q), (q, q // 2), (q + q // 2, q // 2))

    def summed(d, i):
        place, size = cuts[i]
        src = at(ov, 2, (2 * (place // q) + d) * q + place % q, size)
        return remote(src, at(fv, d, first(d, 0) + place, size), sums_sent, sum_recv.at[i], to[d])

    def load(slot, parts):
        out, place = [], 0
        for src, size in parts:
            out.append(pltpu.make_async_copy(src, xv.at[slot, pl.ds(place, size), :], x_sem.at[slot]))
            place += size
        return out

    def near(core):
        return [(at(xg, device(-1, core), 0, h), h), (at(xg, device(1, core), h, h), h)]

    def opposite(core):
        return [(xg.at[device(2, core)], rows)]

    def late(core):
        a, b = device(1, core), device(-1, core)
        return [(at(xg, a, 0, q), q), (at(xg, b, h, q), q), (at(xg, a, q, q), q), (at(xg, b, h + q, q), q)]

    def start(copies):
        for copy in copies:
            copy.start()

    def wait(copies):
        for copy in copies:
            copy.wait()

    def loaded(slot):
        landed(x_sem.at[slot], rows)

    nt = split(ff, 768)
    dt = split(depth, 2048)

    def weights(i):
        r = pl.ds(pl.multiple_of(i * nt, nt), nt)
        return [
            pltpu.make_async_copy(wg.at[:, r], wgv.at[:, r], w_sem.at[0, i]),
            pltpu.make_async_copy(wu.at[:, r], wuv.at[:, r], w_sem.at[1, i]),
        ]

    down = pltpu.make_async_copy(wd, wdv, wd_sem)

    def up(slot, hslot, hook=None, arriving=False):
        def body(i, carry):
            if arriving:
                wait(weights(i))
            if hook is not None:
                pl.when(i == ff // nt - 1)(hook)
            for s in range(0, nt, 256):
                r = pl.ds(pl.multiple_of(i * nt + s, 256), 256)
                a = xv[slot]
                g = jnp.dot(a, wgv[:, r], preferred_element_type=F32)
                u = jnp.dot(a, wuv[:, r], preferred_element_type=F32)
                hv[hslot, :, r] = (g * jax.nn.sigmoid(g) * u).astype(BF16)
            return carry

        lax.fori_loop(0, ff // nt, body, 0)

    def project(hslot, place, size, finish, hook=None):
        def body(i, carry):
            if hook is not None:
                pl.when(i == depth // dt - 1)(hook)
            for s in range(0, dt, 512):
                r = pl.ds(pl.multiple_of(i * dt + s, 512), 512)
                finish(r, jnp.dot(hv[hslot, pl.ds(place, size), :], wdv[:, r], preferred_element_type=F32))
            return carry

        lax.fori_loop(0, depth // dt, body, 0)

    def to_other(slot):
        def finish(r, acc):
            ov[slot, :, r] = acc.astype(BF16)
        return finish

    def to_own(r, acc):
        own[:, r] = acc + tv[0, :, r].astype(F32)

    def to_ring(slot, j):
        def finish(r, acc):
            ov[slot, :, r] = (acc + tv[j % 2, :, r].astype(F32)).astype(BF16)
        return finish

    def to_last(j):
        def finish(r, acc):
            for d in (0, 1):
                place = pl.ds((2 * j + d) * q, q)
                total = acc[d * q:(d + 1) * q] + tv[1, place, r].astype(F32) + sv[d, pl.ds(j * q, q), r].astype(F32)
                ov[2, place, r] = total.astype(BF16)
        return finish

    barrier = pltpu.get_barrier_semaphore()
    for device_id in (right, left, partner):
        pl.semaphore_signal(barrier, inc=1, device_id={AXIS: device_id}, device_id_type=MESH)
    load_own = load(0, [(x, rows)])
    start(load_own)
    for i in range(ff // nt):
        start(weights(i))
    down.start()

    pl.semaphore_wait(barrier, 3)

    ag_start(0, 1)
    xd(0).start()

    xd_wait(0)
    load_partner = load(1, [(xg.at[partner], rows)])
    start(load_partner)
    loaded(0)
    up(0, 0, arriving=True)

    ag_wait(0)
    ag_start(2)
    loaded(1)
    up(1, 1)
    down.wait()
    project(1, 0, rows, to_other(0))
    td(0, 0).start()

    ag_wait(1)
    ag_start(3, 4)
    xd(1).start()
    xd(2).start()
    tile = load(0, near(k))
    start(tile)
    tile_other = load(1, near(other))

    def hook_near():
        xd_wait(1)
        start(tile_other)

    loaded(0)
    up(0, 1, hook_near)
    td(0, 0).wait_recv()
    project(0, 0, rows, to_own)
    loaded(1)
    up(1, 0)
    project(0, 0, rows, to_other(1))
    td(1, 1).start()

    ag_wait(2)
    xd(3).start()
    xd(4).start()
    tile_other2 = load(0, opposite(other))

    def hook_far():
        xd_wait(2)
        start(tile_other2)

    td(1, 1).wait_recv()
    project(1, 0, rows, to_ring(2, 1), hook_far)
    direct(0).start()
    direct(1).start()

    tile2 = load(1, opposite(k))
    start(tile2)
    loaded(0)
    up(0, 0)
    td(0, 0).wait_send()
    project(0, 0, rows, to_other(0))
    td(2, 0).start()
    loaded(1)
    up(1, 1)

    ag_wait(3)
    xd(5).start()
    xd(6).start()
    td(2, 0).wait_recv()
    td(1, 1).wait_send()
    tile_other3 = load(0, late(other))

    def hook_late():
        xd_wait(3)
        start(tile_other3)

    project(1, 0, rows, to_ring(1, 2), hook_late)
    for j in (0, 1):
        for d in (0, 1):
            distant(d, j).start()

    tile3 = load(1, late(k))
    start(tile3)
    loaded(0)
    up(0, 0)
    td(2, 0).wait_send()
    project(0, 0, rows, to_other(0))
    td(3, 0).start()
    loaded(1)
    up(1, 1)
    td(3, 0).wait_recv()
    landed(dir_send, rows)

    for j in (0, 1):
        landed(far_recv.at[j], 2 * q)
        project(1, 2 * j * q, 2 * q, to_last(j))
        for i in (0,) if j == 0 else (1, 2):
            for d in (0, 1):
                summed(d, i).start()

    td(3, 0).wait_send()
    landed(rows_sent, 3 * rows + 4 * rows)
    landed(dir_recv, rows)
    for i, (place, size) in enumerate(cuts):
        landed(sum_recv.at[i], 2 * size)
        for d in (0, 1):
            r = pl.ds(first(d, 0) + place, size)
            y[r, :] = (own[r, :] + fv[0, r, :].astype(F32) + fv[1, r, :].astype(F32)).astype(BF16)
    landed(sums_sent, 2 * rows)


def solution(mesh):
    n = mesh.shape[AXIS]

    def step(x, w_gate, w_up, w_down):
        rows, depth = x.shape
        ff = w_gate.shape[1]
        any_space = pl.BlockSpec(memory_space=pl.ANY)
        dma = pltpu.SemaphoreType.DMA
        out = pl.pallas_call(
            functools.partial(kernel, n),
            out_shape=(
                pltpu.VMEM((rows, depth), BF16),
                jax.ShapeDtypeStruct((n, rows, depth), BF16),
            ),
            in_specs=[any_space] * 4,
            out_specs=(pl.BlockSpec(memory_space=pltpu.VMEM), any_space),
            scratch_shapes=[
                pltpu.VMEM((depth, ff), BF16),
                pltpu.VMEM((depth, ff), BF16),
                pltpu.VMEM((ff, depth), BF16),
                pltpu.VMEM((2, rows, depth), BF16),
                pltpu.VMEM((2, rows, ff), BF16),
                pltpu.VMEM((3, rows, depth), BF16),
                pltpu.VMEM((2, rows, depth), BF16),
                pltpu.VMEM((2, rows // 2, depth), BF16),
                pltpu.VMEM((2, rows, depth), BF16),
                pltpu.VMEM((rows, depth), F32),
                dma((2, ff // split(ff, 768))), dma, dma((2,)), dma, dma,
                dma((4,)), dma((4,)), dma((2,)), dma((4,)), dma, dma, dma((2,)), dma((3,)),
            ],
            compiler_params=pltpu.CompilerParams(
                collective_id=0, has_side_effects=True, vmem_limit_bytes=VMEM_BYTES
            ),
            name="mlp_block",
        )(x, w_gate, w_up, w_down)
        return out[0]

    return jax.shard_map(
        step,
        mesh=mesh,
        in_specs=(P(("dp", "tp"), None), P(None, "tp"), P(None, "tp"), P("tp", None)),
        out_specs=P(("dp", "tp"), None),
        check_vma=False,
    )
```

```python
import functools

import jax
import jax.numpy as jnp
from jax import lax
from jax.experimental import pallas as pl
from jax.experimental.pallas import tpu as pltpu
from jax.sharding import PartitionSpec as P

MESH = pl.DeviceIdType.MESH
AXIS = "tp"
F32 = jnp.float32
BF16 = jnp.bfloat16
VMEM_BYTES = 67043328 - 2 * 1024 * 1024


def split(total, most):
    return max(t for t in range(256, min(total, most) + 1, 256) if total % t == 0)


def kernel(
    n,
    x, wg, wu, wd,
    y, xg,
    wgv, wuv, wdv, xv, hv, ov, tv, sv, fv, own,
    w_sem, wd_sem, x_sem, rows_sent, sums_sent,
    ag_recv, xd_recv, td_send, td_recv, dir_send, dir_recv, far_recv, sum_recv,
):
    rows, depth = x.shape
    ff = wg.shape[1]
    h, q = rows // 2, rows // 4
    me = lax.axis_index(AXIS)
    chips = n // 2
    c, k = lax.div(me, 2), lax.rem(me, 2)

    def device(step, core):
        return lax.rem(c + step + chips, chips) * 2 + core

    other = 1 - k
    partner = device(0, other)
    right, left = device(1, k), device(-1, k)
    to = (right, left)
    came = (left, right)

    def at(ref, block, start, size):
        return ref.at[block, pl.ds(start, size), :]

    def remote(src, dst, ssem, rsem, device_id):
        return pltpu.make_async_remote_copy(
            src_ref=src, dst_ref=dst, send_sem=ssem, recv_sem=rsem,
            device_id={AXIS: device_id}, device_id_type=MESH,
        )

    def landed(sem, count):
        if count % rows == 0:
            ref = xg.at[pl.ds(0, count // rows)]
        else:
            ref = at(xg, 0, 0, count)
        pltpu.make_async_copy(ref, ref, sem).wait()

    def first(d, j):
        return (0 if d == 0 else h) + j * q

    def second(d, j):
        return (h if d == 0 else 0) + j * q

    def ag(d, t):
        if t in (2, 3):
            r = pl.ds(first(d, t - 2), q)
            src = xg.at[came[d], r, :]
            dst = src
        else:
            r = pl.ds(first(d, t), q) if t < 2 else pl.ds(second(d, 0), h)
            src = x.at[r, :]
            dst = xg.at[me, r, :]
        return remote(src, dst, rows_sent, ag_recv.at[(0, 1, 2, 2, 3)[t]], to[d])

    def ag_wait(i):
        landed(ag_recv.at[i], (2 * q, 2 * q, 4 * q, 2 * h)[i])

    def ag_start(*ts):
        for t in ts:
            for d in (0, 1):
                ag(d, t).start()

    far = device(2, k)
    pieces = ((left, 0), (right, h), (far, 0), (far, h), (left, h), (right, 0))

    def xd(i):
        if i == 0:
            src, dst = x, xg.at[me]
        else:
            block, start = pieces[i - 1]
            src = at(xg, block, start, h)
            dst = src
        return remote(src, dst, rows_sent, xd_recv.at[(i + 1) // 2], partner)

    def xd_wait(i):
        landed(xd_recv.at[i], rows)

    def td(j, slot):
        return remote(ov.at[slot], tv.at[j % 2], td_send, td_recv.at[j % 2], partner)

    def direct(d):
        r = pl.ds(h, h) if d == 0 else pl.ds(0, h)
        return remote(ov.at[2, r, :], fv.at[d, r, :], dir_send, dir_recv, to[d])

    def distant(d, j):
        return remote(at(ov, 1, first(d, j), q), at(sv, d, j * q, q), sums_sent, far_recv.at[j], to[d])

    cuts = ((0, q), (q, 3 * q // 4), (q + 3 * q // 4, q // 4))

    def summed(d, i):
        place, size = cuts[i]
        src = at(ov, 2, (2 * (place // q) + d) * q + place % q, size)
        return remote(src, at(fv, d, first(d, 0) + place, size), sums_sent, sum_recv.at[i], to[d])

    def load(slot, parts):
        out, place = [], 0
        for src, size in parts:
            out.append(pltpu.make_async_copy(src, xv.at[slot, pl.ds(place, size), :], x_sem.at[slot]))
            place += size
        return out

    def near(core):
        return [(at(xg, device(-1, core), 0, h), h), (at(xg, device(1, core), h, h), h)]

    def opposite(core):
        return [(xg.at[device(2, core)], rows)]

    def late(core):
        a, b = device(1, core), device(-1, core)
        return [(at(xg, a, 0, q), q), (at(xg, b, h, q), q), (at(xg, a, q, q), q), (at(xg, b, h + q, q), q)]

    def start(copies):
        for copy in copies:
            copy.start()

    def wait(copies):
        for copy in copies:
            copy.wait()

    def loaded(slot):
        landed(x_sem.at[slot], rows)

    nt = split(ff, 768)
    dt = split(depth, 2048)

    def weights(i):
        r = pl.ds(pl.multiple_of(i * nt, nt), nt)
        return [
            pltpu.make_async_copy(wg.at[:, r], wgv.at[:, r], w_sem.at[i]),
            pltpu.make_async_copy(wu.at[:, r], wuv.at[:, r], w_sem.at[i]),
        ]

    down = pltpu.make_async_copy(wd, wdv, wd_sem)

    def up(slot, hslot, hook=None, arriving=False):
        def body(i, carry):
            if arriving:
                both = wgv.at[:, pl.ds(0, 2 * nt)]
                pltpu.make_async_copy(both, both, w_sem.at[i]).wait()
            if hook is not None:
                pl.when(i == ff // nt - 1)(hook)
            for s in range(0, nt, 256):
                r = pl.ds(pl.multiple_of(i * nt + s, 256), 256)
                a = xv[slot]
                g = jnp.dot(a, wgv[:, r], preferred_element_type=F32)
                u = jnp.dot(a, wuv[:, r], preferred_element_type=F32)
                hv[hslot, :, r] = (g * jax.nn.sigmoid(g) * u).astype(BF16)
            return carry

        lax.fori_loop(0, ff // nt, body, 0)

    def project(hslot, place, size, finish, hook=None):
        def body(i, carry):
            if hook is not None:
                pl.when(i == depth // dt - 1)(hook)
            for s in range(0, dt, 512):
                r = pl.ds(pl.multiple_of(i * dt + s, 512), 512)
                finish(r, jnp.dot(hv[hslot, pl.ds(place, size), :], wdv[:, r], preferred_element_type=F32))
            return carry

        lax.fori_loop(0, depth // dt, body, 0)

    def to_other(slot):
        def finish(r, acc):
            ov[slot, :, r] = acc.astype(BF16)
        return finish

    def to_own(r, acc):
        own[:, r] = acc + tv[0, :, r].astype(F32)

    def to_ring(slot, j):
        def finish(r, acc):
            ov[slot, :, r] = (acc + tv[j % 2, :, r].astype(F32)).astype(BF16)
        return finish

    def to_last(j):
        def finish(r, acc):
            for d in (0, 1):
                place = pl.ds((2 * j + d) * q, q)
                total = acc[d * q:(d + 1) * q] + tv[1, place, r].astype(F32) + sv[d, pl.ds(j * q, q), r].astype(F32)
                ov[2, place, r] = total.astype(BF16)
        return finish

    barrier = pltpu.get_barrier_semaphore()
    for device_id in (right, left, partner):
        pl.semaphore_signal(barrier, inc=1, device_id={AXIS: device_id}, device_id_type=MESH)
    load_own = load(0, [(x, rows)])
    start(load_own)
    for i in range(ff // nt):
        start(weights(i))
    down.start()

    pl.semaphore_wait(barrier, 3)

    ag_start(0, 1)
    xd(0).start()

    xd_wait(0)
    load_partner = load(1, [(xg.at[partner], rows)])
    start(load_partner)
    loaded(0)
    up(0, 0, arriving=True)

    ag_wait(0)
    ag_start(2)
    loaded(1)
    up(1, 1)
    down.wait()
    project(1, 0, rows, to_other(0))
    td(0, 0).start()

    ag_wait(1)
    ag_start(3, 4)
    xd(1).start()
    xd(2).start()
    tile = load(0, near(k))
    start(tile)
    tile_other = load(1, near(other))

    def hook_near():
        xd_wait(1)
        start(tile_other)

    loaded(0)
    up(0, 1, hook_near)
    td(0, 0).wait_recv()
    project(0, 0, rows, to_own)
    loaded(1)
    up(1, 0)
    project(0, 0, rows, to_other(1))
    td(0, 0).wait_send()
    td(1, 1).start()

    ag_wait(2)
    xd(3).start()
    xd(4).start()
    tile_other2 = load(0, opposite(other))

    def hook_far():
        xd_wait(2)
        start(tile_other2)

    td(1, 1).wait_recv()
    project(1, 0, rows, to_ring(2, 1), hook_far)
    direct(0).start()
    direct(1).start()

    tile2 = load(1, opposite(k))
    start(tile2)
    loaded(0)
    up(0, 0)
    project(0, 0, rows, to_other(0))
    td(1, 1).wait_send()
    td(2, 0).start()
    loaded(1)
    up(1, 1)

    ag_wait(3)
    xd(5).start()
    xd(6).start()
    td(2, 0).wait_recv()
    tile_other3 = load(0, late(other))

    def hook_late():
        xd_wait(3)
        start(tile_other3)

    project(1, 0, rows, to_ring(1, 2), hook_late)
    for j in (0, 1):
        for d in (0, 1):
            distant(d, j).start()

    tile3 = load(1, late(k))
    start(tile3)
    loaded(0)
    up(0, 0)
    td(2, 0).wait_send()
    project(0, 0, rows, to_other(0))
    td(3, 0).start()
    loaded(1)
    up(1, 1)
    td(3, 0).wait_recv()
    landed(dir_send, rows)

    for j in (0, 1):
        landed(far_recv.at[j], 2 * q)
        project(1, 2 * j * q, 2 * q, to_last(j))
        for i in (0,) if j == 0 else (1, 2):
            for d in (0, 1):
                summed(d, i).start()

    td(3, 0).wait_send()
    landed(rows_sent, 3 * rows + 4 * rows)
    landed(dir_recv, rows)
    for i, (place, size) in enumerate(cuts):
        landed(sum_recv.at[i], 2 * size)
        for d in (0, 1):
            r = pl.ds(first(d, 0) + place, size)
            y[r, :] = (own[r, :] + fv[0, r, :].astype(F32) + fv[1, r, :].astype(F32)).astype(BF16)
    landed(sums_sent, 2 * rows)


def solution(mesh):
    n = mesh.shape[AXIS]

    def step(x, w_gate, w_up, w_down):
        rows, depth = x.shape
        ff = w_gate.shape[1]
        any_space = pl.BlockSpec(memory_space=pl.ANY)
        dma = pltpu.SemaphoreType.DMA
        out = pl.pallas_call(
            functools.partial(kernel, n),
            out_shape=(
                pltpu.VMEM((rows, depth), BF16),
                jax.ShapeDtypeStruct((n, rows, depth), BF16),
            ),
            in_specs=[any_space] * 4,
            out_specs=(pl.BlockSpec(memory_space=pltpu.VMEM), any_space),
            scratch_shapes=[
                pltpu.VMEM((depth, ff), BF16),
                pltpu.VMEM((depth, ff), BF16),
                pltpu.VMEM((ff, depth), BF16),
                pltpu.VMEM((2, rows, depth), BF16),
                pltpu.VMEM((2, rows, ff), BF16),
                pltpu.VMEM((3, rows, depth), BF16),
                pltpu.VMEM((2, rows, depth), BF16),
                pltpu.VMEM((2, rows // 2, depth), BF16),
                pltpu.VMEM((2, rows, depth), BF16),
                pltpu.VMEM((rows, depth), F32),
                dma((ff // split(ff, 768),)), dma, dma((2,)), dma, dma,
                dma((4,)), dma((4,)), dma, dma((2,)), dma, dma, dma((2,)), dma((3,)),
            ],
            compiler_params=pltpu.CompilerParams(
                collective_id=0, has_side_effects=True, vmem_limit_bytes=VMEM_BYTES
            ),
            name="mlp_block",
        )(x, w_gate, w_up, w_down)
        return out[0]

    return jax.shard_map(
        step,
        mesh=mesh,
        in_specs=(P(("dp", "tp"), None), P(None, "tp"), P(None, "tp"), P("tp", None)),
        out_specs=P(("dp", "tp"), None),
        check_vma=False,
    )
```

```python
import functools

import jax
import jax.numpy as jnp
from jax import lax
from jax.experimental import pallas as pl
from jax.experimental.pallas import tpu as pltpu
from jax.sharding import PartitionSpec as P

MESH = pl.DeviceIdType.MESH
AXIS = "tp"
F32 = jnp.float32
BF16 = jnp.bfloat16
VMEM_BYTES = 67043328 - 2 * 1024 * 1024


def split(total, most):
    return max(t for t in range(256, min(total, most) + 1, 256) if total % t == 0)


def kernel(
    n,
    x, wg, wu, wd,
    y, xg,
    wgv, wuv, wdv, xv, hv, ov, tv, sv, fv, own,
    w_sem, x_sem, rows_sent, sums_sent, ag_recv, xd_recv, td_send, td_recv, dir_recv,
):
    rows, depth = x.shape
    ff = wg.shape[1]
    h, q = rows // 2, rows // 4
    me = lax.axis_index(AXIS)
    chips = n // 2
    c, k = lax.div(me, 2), lax.rem(me, 2)

    def device(step, core):
        return lax.rem(c + step + chips, chips) * 2 + core

    other = 1 - k
    partner = device(0, other)
    right, left = device(1, k), device(-1, k)
    to = (right, left)
    came = (left, right)

    def at(ref, block, start, size):
        return ref.at[block, pl.ds(start, size), :]

    def remote(src, dst, ssem, rsem, device_id):
        return pltpu.make_async_remote_copy(
            src_ref=src, dst_ref=dst, send_sem=ssem, recv_sem=rsem,
            device_id={AXIS: device_id}, device_id_type=MESH,
        )

    def landed(sem, count):
        if count % rows == 0:
            ref = xg.at[pl.ds(0, count // rows)]
        else:
            ref = at(xg, 0, 0, count)
        pltpu.make_async_copy(ref, ref, sem).wait()

    def first(d, j):
        return (0 if d == 0 else h) + j * q

    def second(d, j):
        return (h if d == 0 else 0) + j * q

    def ag(d, t):
        if t in (2, 3):
            r = pl.ds(first(d, t - 2), q)
            src = xg.at[came[d], r, :]
            dst = src
        else:
            r = pl.ds(first(d, t), q) if t < 2 else pl.ds(second(d, 0), h)
            src = x.at[r, :]
            dst = xg.at[me, r, :]
        return remote(src, dst, rows_sent, ag_recv.at[(0, 1, 2, 2, 3)[t]], to[d])

    def ag_wait(i):
        landed(ag_recv.at[i], (2 * q, 2 * q, 4 * q, 2 * h)[i])

    def ag_start(*ts):
        for t in ts:
            for d in (0, 1):
                ag(d, t).start()

    far = device(2, k)
    pieces = ((left, 0), (right, h), (far, 0), (far, h), (left, h), (right, 0))

    def xd(i):
        if i == 0:
            src, dst = x, xg.at[me]
        else:
            block, start = pieces[i - 1]
            src = at(xg, block, start, h)
            dst = src
        return remote(src, dst, rows_sent, xd_recv.at[(i + 1) // 2 % 2], partner)

    def xd_wait(i):
        landed(xd_recv.at[i % 2], rows)

    def td(j, slot):
        return remote(ov.at[slot], tv.at[j % 2], td_send, td_recv.at[j % 2], partner)

    def direct(d):
        r = pl.ds(h, h) if d == 0 else pl.ds(0, h)
        return remote(ov.at[2, r, :], fv.at[d, r, :], rows_sent, dir_recv, to[d])

    def distant(d, j):
        return remote(at(ov, 1, first(d, j), q), at(sv, d, j * q, q), sums_sent, ag_recv.at[j], to[d])

    sum_recv = (ag_recv.at[2], ag_recv.at[3], xd_recv.at[0])
    cuts = ((0, q), (q, 3 * q // 4), (q + 3 * q // 4, q // 4))

    def summed(d, i):
        place, size = cuts[i]
        src = at(ov, 2, (2 * (place // q) + d) * q + place % q, size)
        return remote(src, at(fv, d, first(d, 0) + place, size), sums_sent, sum_recv[i], to[d])

    def load(slot, parts):
        out, place = [], 0
        for src, size in parts:
            out.append(pltpu.make_async_copy(src, xv.at[slot, pl.ds(place, size), :], x_sem))
            place += size
        return out

    def near(core):
        return [(at(xg, device(-1, core), 0, h), h), (at(xg, device(1, core), h, h), h)]

    def opposite(core):
        return [(xg.at[device(2, core)], rows)]

    def late(core):
        a, b = device(1, core), device(-1, core)
        return [(at(xg, a, 0, q), q), (at(xg, b, h, q), q), (at(xg, a, q, q), q), (at(xg, b, h + q, q), q)]

    def start(copies):
        for copy in copies:
            copy.start()

    def wait(copies):
        for copy in copies:
            copy.wait()

    def loaded():
        landed(x_sem, rows)

    nt = split(ff, 768)
    dt = split(depth, 2048)

    def weights(i):
        r = pl.ds(pl.multiple_of(i * nt, nt), nt)
        return [
            pltpu.make_async_copy(wg.at[:, r], wgv.at[:, r], w_sem.at[i]),
            pltpu.make_async_copy(wu.at[:, r], wuv.at[:, r], w_sem.at[i]),
        ]

    down = pltpu.make_async_copy(wd, wdv, w_sem.at[0])

    def up(slot, hslot, hook=None, arriving=False):
        def body(i, carry):
            if arriving:
                both = wgv.at[:, pl.ds(0, 2 * nt)]
                pltpu.make_async_copy(both, both, w_sem.at[i]).wait()
                pl.when(i == 0)(down.start)
            if hook is not None:
                pl.when(i == ff // nt - 1)(hook)
            for s in range(0, nt, 256):
                r = pl.ds(pl.multiple_of(i * nt + s, 256), 256)
                a = xv[slot]
                g = jnp.dot(a, wgv[:, r], preferred_element_type=F32)
                u = jnp.dot(a, wuv[:, r], preferred_element_type=F32)
                hv[hslot, :, r] = (g * jax.nn.sigmoid(g) * u).astype(BF16)
            return carry

        lax.fori_loop(0, ff // nt, body, 0)

    def project(hslot, place, size, finish, hook=None):
        def body(i, carry):
            if hook is not None:
                pl.when(i == depth // dt - 1)(hook)
            for s in range(0, dt, 512):
                r = pl.ds(pl.multiple_of(i * dt + s, 512), 512)
                finish(r, jnp.dot(hv[hslot, pl.ds(place, size), :], wdv[:, r], preferred_element_type=F32))
            return carry

        lax.fori_loop(0, depth // dt, body, 0)

    def to_other(slot):
        def finish(r, acc):
            ov[slot, :, r] = acc.astype(BF16)
        return finish

    def to_own(r, acc):
        own[:, r] = acc + tv[0, :, r].astype(F32)

    def to_ring(slot, j):
        def finish(r, acc):
            ov[slot, :, r] = (acc + tv[j % 2, :, r].astype(F32)).astype(BF16)
        return finish

    def to_last(j):
        def finish(r, acc):
            for d in (0, 1):
                place = pl.ds((2 * j + d) * q, q)
                total = acc[d * q:(d + 1) * q] + tv[1, place, r].astype(F32) + sv[d, pl.ds(j * q, q), r].astype(F32)
                ov[2, place, r] = total.astype(BF16)
        return finish

    barrier = pltpu.get_barrier_semaphore()
    for device_id in (right, left, partner):
        pl.semaphore_signal(barrier, inc=1, device_id={AXIS: device_id}, device_id_type=MESH)
    load_own = load(0, [(x, rows)])
    start(load_own)
    for i in range(ff // nt):
        start(weights(i))

    pl.semaphore_wait(barrier, 3)

    ag_start(0, 1)
    xd(0).start()

    xd_wait(0)
    load_partner = load(1, [(xg.at[partner], rows)])
    loaded()
    start(load_partner)
    up(0, 0, arriving=True)

    ag_wait(0)
    ag_start(2)
    loaded()
    up(1, 1)
    down.wait()
    project(1, 0, rows, to_other(0))
    td(0, 0).start()

    ag_wait(1)
    ag_start(3, 4)
    xd(1).start()
    xd(2).start()
    tile = load(0, near(k))
    start(tile)
    tile_other = load(1, near(other))

    def hook_near():
        xd_wait(1)
        start(tile_other)

    loaded()
    up(0, 1, hook_near)
    td(0, 0).wait_recv()
    project(0, 0, rows, to_own)
    loaded()
    up(1, 0)
    project(0, 0, rows, to_other(1))
    td(0, 0).wait_send()
    td(1, 1).start()

    ag_wait(2)
    xd(3).start()
    xd(4).start()
    tile_other2 = load(0, opposite(other))

    def hook_far():
        xd_wait(2)
        start(tile_other2)

    td(1, 1).wait_recv()
    project(1, 0, rows, to_ring(2, 1), hook_far)
    direct(0).start()
    direct(1).start()

    tile2 = load(1, opposite(k))
    loaded()
    start(tile2)
    up(0, 0)
    project(0, 0, rows, to_other(0))
    td(1, 1).wait_send()
    td(2, 0).start()
    loaded()
    up(1, 1)

    ag_wait(3)
    xd(5).start()
    xd(6).start()
    td(2, 0).wait_recv()
    tile_other3 = load(0, late(other))

    def hook_late():
        xd_wait(3)
        start(tile_other3)

    project(1, 0, rows, to_ring(1, 2), hook_late)
    for j in (0, 1):
        for d in (0, 1):
            distant(d, j).start()

    tile3 = load(1, late(k))
    loaded()
    start(tile3)
    up(0, 0)
    td(2, 0).wait_send()
    project(0, 0, rows, to_other(0))
    td(3, 0).start()
    loaded()
    up(1, 1)
    td(3, 0).wait_recv()
    landed(rows_sent, (3 + 4 + 1) * rows)

    for j in (0, 1):
        landed(ag_recv.at[j], 2 * q)
        project(1, 2 * j * q, 2 * q, to_last(j))
        for i in (0,) if j == 0 else (1, 2):
            for d in (0, 1):
                summed(d, i).start()

    td(3, 0).wait_send()
    landed(dir_recv, rows)
    for i, (place, size) in enumerate(cuts):
        landed(sum_recv[i], 2 * size)
        for d in (0, 1):
            r = pl.ds(first(d, 0) + place, size)
            y[r, :] = (own[r, :] + fv[0, r, :].astype(F32) + fv[1, r, :].astype(F32)).astype(BF16)
    landed(sums_sent, 2 * rows)


def solution(mesh):
    n = mesh.shape[AXIS]

    def step(x, w_gate, w_up, w_down):
        rows, depth = x.shape
        ff = w_gate.shape[1]
        any_space = pl.BlockSpec(memory_space=pl.ANY)
        dma = pltpu.SemaphoreType.DMA
        out = pl.pallas_call(
            functools.partial(kernel, n),
            out_shape=(
                pltpu.VMEM((rows, depth), BF16),
                jax.ShapeDtypeStruct((n, rows, depth), BF16),
            ),
            in_specs=[any_space] * 4,
            out_specs=(pl.BlockSpec(memory_space=pltpu.VMEM), any_space),
            scratch_shapes=[
                pltpu.VMEM((depth, ff), BF16),
                pltpu.VMEM((depth, ff), BF16),
                pltpu.VMEM((ff, depth), BF16),
                pltpu.VMEM((2, rows, depth), BF16),
                pltpu.VMEM((2, rows, ff), BF16),
                pltpu.VMEM((3, rows, depth), BF16),
                pltpu.VMEM((2, rows, depth), BF16),
                pltpu.VMEM((2, rows // 2, depth), BF16),
                pltpu.VMEM((2, rows, depth), BF16),
                pltpu.VMEM((rows, depth), F32),
                dma((ff // split(ff, 768),)), dma, dma, dma, dma((4,)), dma((2,)), dma, dma((2,)), dma,
            ],
            compiler_params=pltpu.CompilerParams(
                collective_id=0, has_side_effects=True, vmem_limit_bytes=VMEM_BYTES
            ),
            name="mlp_block",
        )(x, w_gate, w_up, w_down)
        return out[0]

    return jax.shard_map(
        step,
        mesh=mesh,
        in_specs=(P(("dp", "tp"), None), P(None, "tp"), P(None, "tp"), P("tp", None)),
        out_specs=P(("dp", "tp"), None),
        check_vma=False,
    )
```

```python
import functools

import jax
import jax.numpy as jnp
from jax import lax
from jax.experimental import pallas as pl
from jax.experimental.pallas import tpu as pltpu
from jax.sharding import PartitionSpec as P

MESH = pl.DeviceIdType.MESH
AXIS = "tp"
F32 = jnp.float32
BF16 = jnp.bfloat16
VMEM_BYTES = 67043328 - 2 * 1024 * 1024


def split(total, most):
    return max(t for t in range(256, min(total, most) + 1, 256) if total % t == 0)


def kernel(
    n,
    x, wg, wu, wd,
    y, xg,
    wgv, wuv, wdv, xv, hv, ov, tv, sv, fv, own,
    w_sem, x_sem, rows_sent, sums_sent, ag_recv, xd_recv, td_send, td_recv, dir_recv,
):
    rows, depth = x.shape
    ff = wg.shape[1]
    h, q = rows // 2, rows // 4
    me = lax.axis_index(AXIS)
    chips = n // 2
    c, k = lax.div(me, 2), lax.rem(me, 2)

    def device(step, core):
        return lax.rem(c + step + chips, chips) * 2 + core

    other = 1 - k
    partner = device(0, other)
    right, left = device(1, k), device(-1, k)
    to = (right, left)
    came = (left, right)

    def at(ref, block, start, size):
        return ref.at[block, pl.ds(start, size), :]

    def remote(src, dst, ssem, rsem, device_id):
        return pltpu.make_async_remote_copy(
            src_ref=src, dst_ref=dst, send_sem=ssem, recv_sem=rsem,
            device_id={AXIS: device_id}, device_id_type=MESH,
        )

    def landed(sem, count):
        if count % rows == 0:
            ref = xg.at[pl.ds(0, count // rows)]
        else:
            ref = at(xg, 0, 0, count)
        pltpu.make_async_copy(ref, ref, sem).wait()

    def first(d, j):
        return (0 if d == 0 else h) + j * q

    def second(d, j):
        return (h if d == 0 else 0) + j * q

    def ag(d, t):
        if t in (2, 3):
            r = pl.ds(first(d, t - 2), q)
            src = xg.at[came[d], r, :]
            dst = src
        else:
            r = pl.ds(first(d, t), q) if t < 2 else pl.ds(second(d, 0), h)
            src = x.at[r, :]
            dst = xg.at[me, r, :]
        return remote(src, dst, rows_sent, ag_recv.at[(0, 1, 2, 2, 3)[t]], to[d])

    def ag_wait(i):
        landed(ag_recv.at[i], (2 * q, 2 * q, 4 * q, 2 * h)[i])

    def ag_start(*ts):
        for t in ts:
            for d in (0, 1):
                ag(d, t).start()

    far = device(2, k)
    pieces = ((left, 0), (right, h), (far, 0), (far, h), (left, h), (right, 0))

    def xd(i):
        if i == 0:
            src, dst = x, xg.at[me]
        else:
            block, start = pieces[i - 1]
            src = at(xg, block, start, h)
            dst = src
        return remote(src, dst, rows_sent, xd_recv.at[(i + 1) // 2 % 2], partner)

    def xd_wait(i):
        landed(xd_recv.at[i % 2], rows)

    def td(j, slot):
        return remote(ov.at[slot], tv.at[j % 2], td_send, w_sem.at[1] if j % 2 else td_recv, partner)

    def direct(d):
        r = pl.ds(h, h) if d == 0 else pl.ds(0, h)
        return remote(ov.at[2, r, :], fv.at[d, r, :], rows_sent, dir_recv, to[d])

    def distant(d, j):
        return remote(at(ov, 1, first(d, j), q), at(sv, d, j * q, q), sums_sent, ag_recv.at[j], to[d])

    sum_recv = (ag_recv.at[2], ag_recv.at[3], xd_recv.at[0])
    cuts = ((0, q), (q, 3 * q // 4), (q + 3 * q // 4, q // 4))

    def summed(d, i):
        place, size = cuts[i]
        src = at(ov, 2, (2 * (place // q) + d) * q + place % q, size)
        return remote(src, at(fv, d, first(d, 0) + place, size), sums_sent, sum_recv[i], to[d])

    def load(slot, parts):
        out, place = [], 0
        for src, size in parts:
            out.append(pltpu.make_async_copy(src, xv.at[slot, pl.ds(place, size), :], x_sem))
            place += size
        return out

    def near(core):
        return [(at(xg, device(-1, core), 0, h), h), (at(xg, device(1, core), h, h), h)]

    def near_part(j):
        return [
            pltpu.make_async_copy(at(xg, came[d], first(d, j), q), at(xv, 0, first(d, j), q), x_sem) for d in (0, 1)
        ]

    def opposite(core):
        return [(xg.at[device(2, core)], rows)]

    def late(core):
        a, b = device(1, core), device(-1, core)
        return [(at(xg, a, 0, q), q), (at(xg, b, h, q), q), (at(xg, a, q, q), q), (at(xg, b, h + q, q), q)]

    def start(copies):
        for copy in copies:
            copy.start()

    def wait(copies):
        for copy in copies:
            copy.wait()

    def loaded():
        landed(x_sem, rows)

    nt = split(ff, 768)
    dt = split(depth, 2048)

    def weights(i):
        r = pl.ds(pl.multiple_of(i * nt, nt), nt)
        return [
            pltpu.make_async_copy(wg.at[:, r], wgv.at[:, r], w_sem.at[i]),
            pltpu.make_async_copy(wu.at[:, r], wuv.at[:, r], w_sem.at[i]),
        ]

    down = pltpu.make_async_copy(wd, wdv, w_sem.at[0])

    def up(slot, hslot, hook=None, arriving=False):
        def body(i, carry):
            if arriving:
                both = wgv.at[:, pl.ds(0, 2 * nt)]
                pltpu.make_async_copy(both, both, w_sem.at[i]).wait()
                pl.when(i == 0)(down.start)
            if hook is not None:
                pl.when(i == ff // nt - 1)(hook)
            for s in range(0, nt, 256):
                r = pl.ds(pl.multiple_of(i * nt + s, 256), 256)
                a = xv[slot]
                g = jnp.dot(a, wgv[:, r], preferred_element_type=F32)
                u = jnp.dot(a, wuv[:, r], preferred_element_type=F32)
                hv[hslot, :, r] = (g * jax.nn.sigmoid(g) * u).astype(BF16)
            return carry

        lax.fori_loop(0, ff // nt, body, 0)

    def project(hslot, place, size, finish, hook=None):
        def body(i, carry):
            if hook is not None:
                pl.when(i == depth // dt - 1)(hook)
            for s in range(0, dt, 512):
                r = pl.ds(pl.multiple_of(i * dt + s, 512), 512)
                finish(r, jnp.dot(hv[hslot, pl.ds(place, size), :], wdv[:, r], preferred_element_type=F32))
            return carry

        lax.fori_loop(0, depth // dt, body, 0)

    def to_other(slot):
        def finish(r, acc):
            ov[slot, :, r] = acc.astype(BF16)
        return finish

    def to_own(r, acc):
        own[:, r] = acc + tv[0, :, r].astype(F32)

    def to_ring(slot, j):
        def finish(r, acc):
            ov[slot, :, r] = (acc + tv[j % 2, :, r].astype(F32)).astype(BF16)
        return finish

    def to_last(j):
        def finish(r, acc):
            for d in (0, 1):
                place = pl.ds((2 * j + d) * q, q)
                total = acc[d * q:(d + 1) * q] + tv[1, place, r].astype(F32) + sv[d, pl.ds(j * q, q), r].astype(F32)
                ov[2, place, r] = total.astype(BF16)
        return finish

    barrier = pltpu.get_barrier_semaphore()
    for device_id in (right, left, partner):
        pl.semaphore_signal(barrier, inc=1, device_id={AXIS: device_id}, device_id_type=MESH)
    load_own = load(0, [(x, rows)])
    start(load_own)
    for i in range(ff // nt):
        start(weights(i))

    pl.semaphore_wait(barrier, 3)

    ag_start(0, 1)
    xd(0).start()

    xd_wait(0)
    load_partner = load(1, [(xg.at[partner], rows)])
    loaded()
    start(load_partner)
    up(0, 0, arriving=True)

    ag_wait(0)
    ag_start(2)
    loaded()
    start(near_part(0))
    up(1, 1)
    down.wait()
    project(1, 0, rows, to_other(0))
    td(0, 0).start()

    ag_wait(1)
    ag_start(3, 4)
    xd(1).start()
    xd(2).start()
    start(near_part(1))
    tile_other = load(1, near(other))

    def hook_near():
        xd_wait(1)
        start(tile_other)

    loaded()
    up(0, 1, hook_near)
    td(0, 0).wait_recv()
    project(0, 0, rows, to_own)
    loaded()
    up(1, 0)
    project(0, 0, rows, to_other(1))
    td(0, 0).wait_send()
    td(1, 1).start()

    ag_wait(2)
    xd(3).start()
    xd(4).start()
    tile_other2 = load(0, opposite(other))

    def hook_far():
        xd_wait(2)
        start(tile_other2)

    td(1, 1).wait_recv()
    project(1, 0, rows, to_ring(2, 1), hook_far)
    direct(0).start()
    direct(1).start()

    tile2 = load(1, opposite(k))
    loaded()
    start(tile2)
    up(0, 0)
    project(0, 0, rows, to_other(0))
    td(1, 1).wait_send()
    td(2, 0).start()
    loaded()
    up(1, 1)

    ag_wait(3)
    xd(5).start()
    xd(6).start()
    td(2, 0).wait_recv()
    tile_other3 = load(0, late(other))

    def hook_late():
        xd_wait(3)
        start(tile_other3)

    project(1, 0, rows, to_ring(1, 2), hook_late)
    for j in (0, 1):
        for d in (0, 1):
            distant(d, j).start()

    tile3 = load(1, late(k))
    loaded()
    start(tile3)
    up(0, 0)
    td(2, 0).wait_send()
    project(0, 0, rows, to_other(0))
    td(3, 0).start()
    loaded()
    up(1, 1)
    td(3, 0).wait_recv()
    landed(rows_sent, (3 + 4 + 1) * rows)

    for j in (0, 1):
        landed(ag_recv.at[j], 2 * q)
        project(1, 2 * j * q, 2 * q, to_last(j))
        for i in (0,) if j == 0 else (1, 2):
            for d in (0, 1):
                summed(d, i).start()

    td(3, 0).wait_send()
    landed(dir_recv, rows)
    for i, (place, size) in enumerate(cuts):
        landed(sum_recv[i], 2 * size)
        for d in (0, 1):
            r = pl.ds(first(d, 0) + place, size)
            y[r, :] = (own[r, :] + fv[0, r, :].astype(F32) + fv[1, r, :].astype(F32)).astype(BF16)
    landed(sums_sent, 2 * rows)


def solution(mesh):
    n = mesh.shape[AXIS]

    def step(x, w_gate, w_up, w_down):
        rows, depth = x.shape
        ff = w_gate.shape[1]
        any_space = pl.BlockSpec(memory_space=pl.ANY)
        dma = pltpu.SemaphoreType.DMA
        out = pl.pallas_call(
            functools.partial(kernel, n),
            out_shape=(
                pltpu.VMEM((rows, depth), BF16),
                jax.ShapeDtypeStruct((n, rows, depth), BF16),
            ),
            in_specs=[any_space] * 4,
            out_specs=(pl.BlockSpec(memory_space=pltpu.VMEM), any_space),
            scratch_shapes=[
                pltpu.VMEM((depth, ff), BF16),
                pltpu.VMEM((depth, ff), BF16),
                pltpu.VMEM((ff, depth), BF16),
                pltpu.VMEM((2, rows, depth), BF16),
                pltpu.VMEM((2, rows, ff), BF16),
                pltpu.VMEM((3, rows, depth), BF16),
                pltpu.VMEM((2, rows, depth), BF16),
                pltpu.VMEM((2, rows // 2, depth), BF16),
                pltpu.VMEM((2, rows, depth), BF16),
                pltpu.VMEM((rows, depth), F32),
                dma((ff // split(ff, 768),)), dma, dma, dma, dma((4,)), dma((2,)), dma, dma, dma,
            ],
            compiler_params=pltpu.CompilerParams(
                collective_id=0, has_side_effects=True, vmem_limit_bytes=VMEM_BYTES
            ),
            name="mlp_block",
        )(x, w_gate, w_up, w_down)
        return out[0]

    return jax.shard_map(
        step,
        mesh=mesh,
        in_specs=(P(("dp", "tp"), None), P(None, "tp"), P(None, "tp"), P("tp", None)),
        out_specs=P(("dp", "tp"), None),
        check_vma=False,
    )
```
